16 devices in a mesh: rep: 4 (over y, z, core), dp: 4 (over x).
Axes of the slice: x: 4, y: 2, z: 1, core: 2. Of those that a mesh axis runs over, the one named last changes fastest.
The devices are a block of a 4x4x8 slice.
Arguments:
- x: bfloat16 [16, 2048, 1024], P(('rep', 'dp')), parts along dimension 0
- dy: bfloat16 [16, 2048, 1024], P(('rep', 'dp')), parts along dimension 0
- wq: bfloat16 [2, 1024, 1024], P(None, 'dp')
- wk: bfloat16 [2, 1024, 256], P(None, 'dp')
- wv: bfloat16 [2, 1024, 256], P(None, 'dp')
- wo: bfloat16 [2, 1024, 1024], P(None, 'dp')
- w_gate: bfloat16 [2, 1024, 3200], P(None, 'dp')
- w_up: bfloat16 [2, 1024, 3200], P(None, 'dp')
- w_down: bfloat16 [2, 3200, 1024], P(None, 'dp')
- m_wq: float32 [2, 1024, 1024], P(None, 'dp')
- m_wk: float32 [2, 1024, 256], P(None, 'dp')
- m_wv: float32 [2, 1024, 256], P(None, 'dp')
- m_wo: float32 [2, 1024, 1024], P(None, 'dp')
- m_w_gate: float32 [2, 1024, 3200], P(None, 'dp')
- m_w_up: float32 [2, 1024, 3200], P(None, 'dp')
- m_w_down: float32 [2, 3200, 1024], P(None, 'dp')
- v_wq: float32 [2, 1024, 1024], P(None, 'dp')
- v_wk: float32 [2, 1024, 256], P(None, 'dp')
- v_wv: float32 [2, 1024, 256], P(None, 'dp')
- v_wo: float32 [2, 1024, 1024], P(None, 'dp')
- v_w_gate: float32 [2, 1024, 3200], P(None, 'dp')
- v_w_up: float32 [2, 1024, 3200], P(None, 'dp')
- v_w_down: float32 [2, 3200, 1024], P(None, 'dp')
Outputs:
- output 1: bfloat16 [8, 1024, 1024], P('rep', 'dp'), parts along dimension 0
- output 2: bfloat16 [8, 1024, 256], P('rep', 'dp'), parts along dimension 0
- output 3: bfloat16 [8, 1024, 256], P('rep', 'dp'), parts along dimension 0
- output 4: bfloat16 [8, 1024, 1024], P('rep', 'dp'), parts along dimension 0
- output 5: bfloat16 [8, 1024, 3200], P('rep', 'dp'), parts along dimension 0
- output 6: bfloat16 [8, 1024, 3200], P('rep', 'dp'), parts along dimension 0
- output 7: bfloat16 [8, 3200, 1024], P('rep', 'dp'), parts along dimension 0
- output 8: float32 [8, 1024, 1024], P('rep', 'dp'), parts along dimension 0
- output 9: float32 [8, 1024, 256], P('rep', 'dp'), parts along dimension 0
- output 10: float32 [8, 1024, 256], P('rep', 'dp'), parts along dimension 0
- output 11: float32 [8, 1024, 1024], P('rep', 'dp'), parts along dimension 0
- output 12: float32 [8, 1024, 3200], P('rep', 'dp'), parts along dimension 0
- output 13: float32 [8, 1024, 3200], P('rep', 'dp'), parts along dimension 0
- output 14: float32 [8, 3200, 1024], P('rep', 'dp'), parts along dimension 0
- output 15: float32 [8, 1024, 1024], P('rep', 'dp'), parts along dimension 0
- output 16: float32 [8, 1024, 256], P('rep', 'dp'), parts along dimension 0
- output 17: float32 [8, 1024, 256], P('rep', 'dp'), parts along dimension 0
- output 18: float32 [8, 1024, 1024], P('rep', 'dp'), parts along dimension 0
- output 19: float32 [8, 1024, 3200], P('rep', 'dp'), parts along dimension 0
- output 20: float32 [8, 1024, 3200], P('rep', 'dp'), parts along dimension 0
- output 21: float32 [8, 3200, 1024], P('rep', 'dp'), parts along dimension 0
There are 4 independent parts. The reference program is written for one: setup_inputs(seed, part) draws one part's arguments, and reference() takes and returns one part's arrays. A program takes and returns all parts, laid end to end along the dimension named above; an argument that names none is the same for every part.
All inputs are finite; a program needn't handle non-finite values.
Results may differ from the reference program's by a relative error of at most 0.027.
Values are sent between devices in bfloat16 or wider.
A program may use at most 768 MiB of HBM per device.

```python
import jax
import jax.numpy as jnp
from jax import lax

SEQUENCES = 4
TOKENS = 2048
D = 1024
HEADS = 8
KV_HEADS = 2
HEAD = 128
FF = 3200
LAYERS = 2
THETA = 10000
NAMES = ("wq", "wk", "wv", "wo", "w_gate", "w_up", "w_down")
SHAPES = {
    "wq": (LAYERS, D, HEADS * HEAD),
    "wk": (LAYERS, D, KV_HEADS * HEAD),
    "wv": (LAYERS, D, KV_HEADS * HEAD),
    "wo": (LAYERS, HEADS * HEAD, D),
    "w_gate": (LAYERS, D, FF),
    "w_up": (LAYERS, D, FF),
    "w_down": (LAYERS, FF, D),
}


def bump(key, n, height):
    away = (jnp.arange(n, dtype=jnp.int32) - jax.random.randint(key, (), 0, n, jnp.int32)) % n
    return jnp.where(away < n // 8, height, 1.0)


def together(key, own, strength):
    shared = jax.random.normal(key, own.shape[1:], jnp.float32)
    return (own + strength * shared) * lax.rsqrt(1 + strength * strength)


def setup_inputs(seed: int = 0, part: int = 0) -> dict:
    kx, kdy, ka, kb, kz, kf, kh, kl, *keys = jax.random.split(jax.random.key(seed), 8 + 3 * len(NAMES))
    kx, kdy, ka, kb = (jax.random.fold_in(k, part) for k in (kx, kdy, ka, kb))
    kw, km, kv = (keys[i::3] for i in range(3))
    shape = (SEQUENCES, TOKENS, D)
    much_x, much_dy = jax.random.uniform(kz, (2,), jnp.float32, 0.0, 1.0)
    loud = 2.0 ** jax.random.uniform(jax.random.fold_in(kz, 1), (), jnp.float32, -1.0, 2.0)
    layers = 2.0 ** jax.random.uniform(kl, (LAYERS, 1, 1), jnp.float32, -1.0, 1.0)
    times = {"wq": 1.0, "wk": 1.0, "wv": 2.0, "wo": layers, "w_gate": 1.0, "w_up": bump(kh, FF, 4.0), "w_down": layers}
    x = together(ka, jax.random.normal(kx, shape, jnp.float32), much_x) * bump(kf, D, 4.0)
    dy = together(kb, jax.random.normal(kdy, shape, jnp.float32), much_dy)
    drawn = {"x": x.astype(jnp.bfloat16), "dy": (loud * dy * (SEQUENCES * TOKENS) ** -0.5).astype(jnp.bfloat16)}
    for key, name in zip(kw, NAMES, strict=True):
        drawn[name] = (jax.random.normal(key, SHAPES[name], jnp.float32) * SHAPES[name][1] ** -0.5 * times[name]).astype(jnp.bfloat16)
    for key, name in zip(km, NAMES, strict=True):
        drawn[f"m_{name}"] = 0.1 * jax.random.normal(key, SHAPES[name], jnp.float32)
    for key, name in zip(kv, NAMES, strict=True):
        drawn[f"v_{name}"] = loud * loud * jax.random.uniform(key, SHAPES[name], jnp.float32, 0.2, 0.6)
    return drawn


def matmul(a, w):
    return jnp.dot(a, w, preferred_element_type=jnp.float32).astype(jnp.bfloat16)


def normed(h):
    wide = h.astype(jnp.float32)
    scale = lax.rsqrt(jnp.mean(wide**2, -1, keepdims=True) + 1e-6)
    return (wide * scale).astype(jnp.bfloat16)


def turned(t, theta):
    half = t.shape[-1] // 2
    angle = jnp.arange(t.shape[0], dtype=jnp.float32)[:, None] * theta ** (-jnp.arange(half, dtype=jnp.float32) / half)
    cos, sin = jnp.cos(angle)[:, None], jnp.sin(angle)[:, None]
    a, b = t[..., :half].astype(jnp.float32), t[..., half:].astype(jnp.float32)
    return jnp.concatenate([a * cos - b * sin, b * cos + a * sin], -1).astype(jnp.bfloat16)


def seen_by(q, k, v):
    tokens, kv = q.shape[0], k.shape[1]
    q = q.reshape(tokens, kv, -1, q.shape[-1])
    scores = jnp.einsum("tgsd,ugd->gstu", q.astype(jnp.float32), k.astype(jnp.float32)) * q.shape[-1] ** -0.5
    place = jnp.arange(tokens)
    weights = jax.nn.softmax(jnp.where(place[:, None] >= place, scores, -jnp.inf), -1).astype(jnp.bfloat16)
    return jnp.einsum("gstu,ugd->tgsd", weights.astype(jnp.float32), v.astype(jnp.float32)).astype(jnp.bfloat16).reshape(tokens, -1)


def layer(h, w):
    a = normed(h)
    q, k = (turned(matmul(a, w[name]).reshape(h.shape[0], -1, HEAD), THETA) for name in ("wq", "wk"))
    h = h + matmul(seen_by(q, k, matmul(a, w["wv"]).reshape(h.shape[0], -1, HEAD)), w["wo"])
    b = normed(h)
    gate = jnp.dot(b, w["w_gate"], preferred_element_type=jnp.float32)
    up = jnp.dot(b, w["w_up"], preferred_element_type=jnp.float32)
    return h + matmul((jax.nn.silu(gate) * up).astype(jnp.bfloat16), w["w_down"])


def adamw(w, m, v, g):
    m = 0.9 * m + 0.1 * g
    v = 0.95 * v + 0.05 * g * g
    step = m * lax.rsqrt(v + 1e-8) + 0.1 * w
    return (w - 0.02 * step).astype(jnp.bfloat16), m, v


def stack(weights, h):
    return lax.scan(lambda h, w: (layer(h, w), None), h, weights)[0]


def reference(x, dy, wq, wk, wv, wo, w_gate, w_up, w_down, m_wq, m_wk, m_wv, m_wo, m_w_gate, m_w_up, m_w_down, v_wq, v_wk, v_wv, v_wo, v_w_gate, v_w_up, v_w_down):
    weights = dict(zip(NAMES, (wq, wk, wv, wo, w_gate, w_up, w_down), strict=True))

    def take(so_far, sequence):
        h, by_y = sequence
        _, back = jax.vjp(stack, weights, h)
        by_weights, by_h = back(by_y)
        return jax.tree.map(lambda total, term: total + term.astype(jnp.float32), so_far, by_weights), by_h

    none_yet = {name: jnp.zeros(w.shape, jnp.float32) for name, w in weights.items()}
    by_weights, by_x = lax.scan(take, none_yet, (x, dy))
    gradients = [by_weights[name].astype(jnp.bfloat16).astype(jnp.float32) for name in NAMES]
    first = (m_wq, m_wk, m_wv, m_wo, m_w_gate, m_w_up, m_w_down)
    second = (v_wq, v_wk, v_wv, v_wo, v_w_gate, v_w_up, v_w_down)
    new = [adamw(weights[name].astype(jnp.float32), m, v, g) for name, m, v, g in zip(NAMES, first, second, gradients, strict=True)]
    return tuple(one[which] for which in range(3) for one in new)
```

```python
import jax
import jax.numpy as jnp
from jax import lax
from jax.experimental import pallas as pl
from jax.experimental.pallas import tpu as pltpu
from jax.sharding import PartitionSpec as P

HEAD = 128
THETA = 10000
LOW = jnp.bfloat16
F32 = jnp.float32
NEG = -1e30
HIDDEN = 2 * NEG
LOG2E = 1.4426950408889634
VMEM = 60 * 2**20
CHUNK = 512


def _dot(a, b, ca=1, cb=0):
    return lax.dot_general(a, b, (((ca,), (cb,)), ((), ())), preferred_element_type=F32)


def _spans(size, width=CHUNK):
    return [(n, min(n + width, size)) for n in range(0, size, width)]


def _call(kernel, grid, ins, outs, args, flops, scratch=(), name=None):
    size = sum(a.size * a.dtype.itemsize for a in args)
    got = pl.pallas_call(
        kernel,
        grid=(grid,),
        in_specs=ins,
        out_specs=[o[2] for o in outs],
        out_shape=[jax.ShapeDtypeStruct(o[0], o[1]) for o in outs],
        scratch_shapes=list(scratch),
        compiler_params=pltpu.CompilerParams(dimension_semantics=("arbitrary",), vmem_limit_bytes=VMEM),
        cost_estimate=pl.CostEstimate(flops=int(flops), transcendentals=0, bytes_accessed=size),
        name=name,
    )(*args)
    return got


def _rows(bm, width, col=0):
    return pl.BlockSpec((bm, width), lambda i, c=col: (i, c))


def _whole(shape, row=0, col=0):
    return pl.BlockSpec(shape, lambda i, r=row, c=col: (r, c), pipeline_mode=pl.Buffered(1))


def _scale(wide):
    return lax.rsqrt(jnp.mean(wide**2, -1, keepdims=True) + 1e-6)


def _norm_back(ct, wide):
    scale = _scale(wide)
    return (ct * scale - wide * (scale * scale * scale * jnp.mean(ct * wide, -1, keepdims=True))).astype(LOW)


def _turn(t, cos, sin):
    t = t.astype(F32)
    return (t * cos + pltpu.roll(t, HEAD // 2, 1) * sin).astype(LOW)


def project(h, wqo, cos, sin, heads, kv, bm=512):
    m, d = h.shape
    nq, nk = heads * HEAD, kv * HEAD
    parts = (nq + 2 * nk) // CHUNK

    def kernel(h_ref, *refs):
        w, (cos_ref, sin_ref, a_ref, q_ref, k_ref, v_ref) = refs[:parts], refs[parts:]
        wide = h_ref[...].astype(F32)
        a = (wide * _scale(wide)).astype(LOW)
        a_ref[...] = a
        cos, sin = cos_ref[...], sin_ref[...]
        for n in range(parts):
            got = _dot(a, w[n][...]).astype(LOW)
            for c in range(0, CHUNK, HEAD):
                at, t = n * CHUNK + c, got[:, c : c + HEAD]
                if at < nq:
                    q_ref[:, at : at + HEAD] = _turn(t, cos, sin)
                elif at < nq + nk:
                    k_ref[:, at - nq : at - nq + HEAD] = _turn(t, cos, sin)
                else:
                    v_ref[:, at - nq - nk : at - nq - nk + HEAD] = t

    return _call(
        kernel, m // bm,
        [_rows(bm, d)] + [_whole((d, CHUNK), 0, n) for n in range(parts)] + [_rows(bm, HEAD)] * 2,
        [((m, d), LOW, _rows(bm, d)), ((m, nq), LOW, _rows(bm, nq)), ((m, nk), LOW, _rows(bm, nk)), ((m, nk), LOW, _rows(bm, nk))],
        [h] + [wqo] * parts + [cos, sin], 2 * m * d * (nq + 2 * nk), name="project")


def _gap(bk, bq):
    return lax.broadcasted_iota(jnp.int32, (bk, bq), 1) - lax.broadcasted_iota(jnp.int32, (bk, bq), 0)


def attend(q, k, v, bq=512, bk=512):
    m, nq = q.shape
    heads, kv = nq // HEAD, k.shape[1] // HEAD
    g = heads // kv
    scale = HEAD**-0.5
    e = scale * LOG2E

    def kernel(q_ref, k_ref, v_ref, o_ref, lse_ref, top_s, mix_s, gap_s):
        iq = pl.program_id(0)

        @pl.when(iq == 0)
        def _():
            gap_s[...] = _gap(bk, bq)

        top_s[...] = jnp.full(top_s.shape, NEG, F32)
        mix_s[...] = jnp.zeros(mix_s.shape, F32)
        ones = jnp.ones((8, bk), LOW)

        def block(j, masked):
            here = pl.ds(pl.multiple_of(j * bk, bk), bk)
            scores = [_dot(k_ref[here, n // g * HEAD : (n // g + 1) * HEAD], q_ref[:, n * HEAD : (n + 1) * HEAD], 1, 1) for n in range(heads)]
            ok = gap_s[...] >= j * bk - iq * bq if masked else None
            weights, keeps = [], []
            for n, s in enumerate(scores):
                if masked:
                    s = jnp.where(ok, s, HIDDEN)
                old = top_s[n : n + 1, :]
                top = jnp.maximum(old, s.max(axis=0, keepdims=True))
                top_s[n : n + 1, :] = top
                weights.append(jnp.exp2((s - top) * e).astype(LOW))
                keeps.append(jnp.exp2((old - top) * e))
            values = [jnp.concatenate([v_ref[here, i * HEAD : (i + 1) * HEAD].T, ones], axis=0) for i in range(kv)]
            for n in range(heads):
                mix_s[n] = mix_s[n] * keeps[n] + _dot(values[n // g], weights[n], 1, 0)

        lax.fori_loop(0, iq * bq // bk, lambda j, _: block(j, False), None)
        lax.fori_loop(iq * bq // bk, (iq + 1) * bq // bk, lambda j, _: block(j, True), None)
        for n in range(heads):
            total = mix_s[n, HEAD : HEAD + 1, :]
            o_ref[:, n * HEAD : (n + 1) * HEAD] = (mix_s[n, :HEAD, :] * (1 / total)).T.astype(LOW)
            lse_ref[n : n + 1, :] = top_s[n : n + 1, :] * scale + jnp.log(total)

    return _call(
        kernel, m // bq,
        [_rows(bq, nq), _whole((m, kv * HEAD)), _whole((m, kv * HEAD))],
        [((m, nq), LOW, _rows(bq, nq)), ((heads, m), F32, pl.BlockSpec((heads, bq), lambda i: (0, i)))],
        [q, k, v], 8 * m * m * nq,
        [pltpu.VMEM((heads, bq), F32), pltpu.VMEM((heads, HEAD + 8, bq), F32), pltpu.VMEM((bk, bq), jnp.int32)], name="attend")


def joined(out, wqo, first, h, bm=512):
    m, d = h.shape
    k = out.shape[1]
    parts = d // CHUNK

    def kernel(o_ref, *refs):
        w, (h_ref, mid_ref, b_ref) = refs[:parts], refs[parts:]
        o = o_ref[...]
        for n in range(parts):
            at = slice(n * CHUNK, (n + 1) * CHUNK)
            mid_ref[:, at] = (h_ref[:, at].astype(F32) + _dot(o, w[n][...]).astype(LOW).astype(F32)).astype(LOW)
        wide = mid_ref[...].astype(F32)
        b_ref[...] = (wide * _scale(wide)).astype(LOW)

    return _call(
        kernel, m // bm,
        [_rows(bm, k)] + [_whole((k, CHUNK), 0, first + n) for n in range(parts)] + [_rows(bm, d)],
        [((m, d), LOW, _rows(bm, d))] * 2, [out] + [wqo] * parts + [h], 2 * m * k * d, name="joined")


def gated(b, wgu, bm=256):
    m, d = b.shape
    f = wgu.shape[1] // 2

    def kernel(b_ref, wg_ref, wu_ref, x_ref, s_ref, t_ref):
        b = b_ref[...]
        for n, e in _spans(f):
            gate, up = _dot(b, wg_ref[:, n:e]), _dot(b, wu_ref[:, n:e])
            sig = jax.nn.sigmoid(gate)
            s = gate * sig
            x_ref[:, n:e] = (s * up).astype(LOW)
            s_ref[:, n:e] = s
            t_ref[:, n:e] = up * (sig * (1 + gate * (1 - sig)))

    return _call(
        kernel, m // bm, [_rows(bm, d), _whole((d, f), 0, 0), _whole((d, f), 0, 1)],
        [((m, f), LOW, _rows(bm, f)), ((m, f), F32, _rows(bm, f)), ((m, f), F32, _rows(bm, f))], [b, wgu, wgu], 4 * m * d * f, name="gated")


def lowered(x, w, h, bm=512):
    m, f = x.shape
    d = h.shape[1]

    def kernel(x_ref, w_ref, h_ref, o_ref):
        x = x_ref[...]
        for n, e in _spans(d):
            o_ref[:, n:e] = (h_ref[:, n:e].astype(F32) + _dot(x, w_ref[:, n:e]).astype(LOW).astype(F32)).astype(LOW)

    return _call(kernel, m // bm, [_rows(bm, f), _whole((f, d)), _rows(bm, d)], [((m, d), LOW, _rows(bm, d))], [x, w, h], 2 * m * f * d,
                 name="lowered")[0]


def outer(a, bs, bm, name):
    t, k = a.shape
    widths = [b.shape[1] for b in bs]
    n = sum(widths)

    def kernel(a_ref, *refs):
        o_ref = refs[-1]
        at = a_ref[...].T
        col = 0
        for b_ref, width in zip(refs, widths):
            for c, e in _spans(width):
                o_ref[:, col + c : col + e] = _dot(at, b_ref[:, c:e]).astype(LOW)
            col += width

    return _call(kernel, k // bm, [pl.BlockSpec((t, bm), lambda i: (0, i))] + [_whole((t, w)) for w in widths],
                 [((k, n), LOW, _rows(bm, n))], [a, *bs], 2 * t * k * n, name=name)[0]


def hidden_back(dh, w, s, t, bm=256):
    m, d = dh.shape
    f = w.shape[0]

    def kernel(dh_ref, w_ref, s_ref, t_ref, dg_ref, du_ref):
        dh = dh_ref[...]
        for n, e in _spans(f):
            dx = _dot(dh, w_ref[n:e, :], 1, 1).astype(LOW).astype(F32)
            dg_ref[:, n:e] = (dx * t_ref[:, n:e]).astype(LOW)
            du_ref[:, n:e] = (dx * s_ref[:, n:e]).astype(LOW)

    return _call(kernel, m // bm, [_rows(bm, d), _whole((f, d)), _rows(bm, f), _rows(bm, f)],
                 [((m, f), LOW, _rows(bm, f)), ((m, f), LOW, _rows(bm, f))], [dh, w, s, t], 2 * m * d * f, name="hidden_back")


def mid_back(dg, du, wgu, mid, dh, bm=256):
    m, f = dg.shape
    d = mid.shape[1]

    def kernel(dg_ref, du_ref, wg_ref, wu_ref, mid_ref, dh_ref, o_ref, db_s):
        dg, du = dg_ref[...], du_ref[...]
        for n, e in _spans(d):
            one, two = _dot(dg, wg_ref[n:e, :], 1, 1).astype(LOW).astype(F32), _dot(du, wu_ref[n:e, :], 1, 1).astype(LOW).astype(F32)
            db_s[:, n:e] = (one + two).astype(LOW).astype(F32)
        o_ref[...] = (dh_ref[...].astype(F32) + _norm_back(db_s[...], mid_ref[...].astype(F32)).astype(F32)).astype(LOW)

    return _call(kernel, m // bm, [_rows(bm, f)] * 2 + [_whole((d, f), 0, 0), _whole((d, f), 0, 1)] + [_rows(bm, d)] * 2,
                 [((m, d), LOW, _rows(bm, d))], [dg, du, wgu, wgu, mid, dh], 4 * m * f * d, [pltpu.VMEM((bm, d), F32)], name="mid_back")[0]


def out_back(dm, wqo, first, bm=512):
    m, d = dm.shape
    k = wqo.shape[0]
    parts = d // CHUNK

    def kernel(dm_ref, *refs):
        w, o_ref = refs[:parts], refs[parts]
        dm = dm_ref[...]
        for n, e in _spans(k):
            o_ref[:, n:e] = sum(_dot(dm[:, p * CHUNK : (p + 1) * CHUNK], w[p][n:e, :], 1, 1) for p in range(parts)).astype(LOW)

    return _call(kernel, m // bm, [_rows(bm, d)] + [_whole((k, CHUNK), 0, first + n) for n in range(parts)],
                 [((m, k), LOW, _rows(bm, k))], [dm] + [wqo] * parts, 2 * m * k * d, name="out_back")[0]


def attend_back(q, k, v, do, out, lse, cos, sin, bq=256, bk=512):
    m, nq = q.shape
    nk = k.shape[1]
    heads, kv = nq // HEAD, nk // HEAD
    g = heads // kv
    cols = g * bq
    scale = HEAD**-0.5
    e = scale * LOG2E
    wide = min(cols, 512)
    pieces = [(i, at) for i in range(kv) for at in range(0, cols, wide)]

    def kernel(q_ref, k_ref, v_ref, do_ref, o_ref, lse_ref, cos_ref, sin_ref, dq_ref, dkv_ref, q_s, do_s, lse_s, delta_s, dq_s, dk_s, dv_s, gap_s):
        iq = pl.program_id(0)

        @pl.when(iq == 0)
        def _():
            gap_s[...] = lax.rem(lax.broadcasted_iota(jnp.int32, (bk, wide), 1), bq) - lax.broadcasted_iota(jnp.int32, (bk, wide), 0)
            dk_s[...] = jnp.zeros(dk_s.shape, F32)
            dv_s[...] = jnp.zeros(dv_s.shape, F32)

        dq_s[...] = jnp.zeros(dq_s.shape, F32)
        for n in range(heads):
            i, at = n // g, n % g * bq
            head = slice(n * HEAD, (n + 1) * HEAD)
            q_s[i, at : at + bq, :] = q_ref[:, head]
            do = do_ref[:, head]
            do_s[i, at : at + bq, :] = do
            lse_s[i : i + 1, at : at + bq] = lse_ref[n : n + 1, :] * LOG2E
            delta_s[i : i + 1, at : at + bq] = (do.astype(F32) * o_ref[:, head].astype(F32)).T.sum(axis=0, keepdims=True)

        def block(j, masked):
            here = pl.ds(pl.multiple_of(j * bk, bk), bk)
            ks = [k_ref[here, i * HEAD : (i + 1) * HEAD] for i in range(kv)]
            vs = [v_ref[here, i * HEAD : (i + 1) * HEAD] for i in range(kv)]
            qs = [q_s[i, at : at + wide, :] for i, at in pieces]
            dos = [do_s[i, at : at + wide, :] for i, at in pieces]
            scores = [_dot(ks[i], x, 1, 1) for (i, _), x in zip(pieces, qs)]
            dps = [_dot(vs[i], x, 1, 1) for (i, _), x in zip(pieces, dos)]
            ok = gap_s[...] >= j * bk - iq * bq if masked else None
            for n, (i, at) in enumerate(pieces):
                p = jnp.exp2(scores[n] * e - lse_s[i : i + 1, at : at + wide])
                if masked:
                    p = jnp.where(ok, p, 0.0)
                ds = (p * (dps[n] - delta_s[i : i + 1, at : at + wide])).astype(LOW)
                dv_s[i, here, :] += _dot(p.astype(LOW), dos[n], 1, 0)
                dk_s[i, here, :] += _dot(ds, qs[n], 1, 0)
                dq_s[i, :, at : at + wide] += _dot(ks[i].T, ds, 1, 0)

        whole = iq * bq // bk
        lax.fori_loop(0, whole, lambda j, _: block(j, False), None)
        block(whole, True)
        place = pl.ds(pl.multiple_of(iq * bq, bq), bq)
        cos, sin = cos_ref[place, :], sin_ref[place, :]
        for n in range(heads):
            i, at = n // g, n % g * bq
            dq_ref[:, n * HEAD : (n + 1) * HEAD] = _turn((dq_s[i, :, at : at + bq] * scale).T.astype(LOW), cos, -sin)

        @pl.when(iq == pl.num_programs(0) - 1)
        def _():
            for i in range(kv):
                dkv_ref[:, i * HEAD : (i + 1) * HEAD] = _turn((dk_s[i] * scale).astype(LOW), cos_ref[...], -sin_ref[...])
                dkv_ref[:, nk + i * HEAD : nk + (i + 1) * HEAD] = dv_s[i].astype(LOW)

    return _call(
        kernel, m // bq,
        [_rows(bq, nq), _whole((m, nk)), _whole((m, nk)), _rows(bq, nq), _rows(bq, nq), pl.BlockSpec((heads, bq), lambda i: (0, i)),
         _whole((m, HEAD)), _whole((m, HEAD))],
        [((m, nq), LOW, _rows(bq, nq)), ((m, 2 * nk), LOW, pl.BlockSpec((m, 2 * nk), lambda i: (0, 0)))],
        [q, k, v, do, out, lse, cos, sin], 14 * m * m * nq,
        [pltpu.VMEM((kv, cols, HEAD), LOW), pltpu.VMEM((kv, cols, HEAD), LOW), pltpu.VMEM((kv, cols), F32), pltpu.VMEM((kv, cols), F32),
         pltpu.VMEM((kv, HEAD, cols), F32), pltpu.VMEM((kv, m, HEAD), F32), pltpu.VMEM((kv, m, HEAD), F32), pltpu.VMEM((bk, wide), jnp.int32)],
        name="attend_back")


def input_back(dq, dkv, wqo, h, dm, bm=512):
    m, d = h.shape
    nq, nk = dq.shape[1], dkv.shape[1] // 2
    parts = (nq + 2 * nk) // CHUNK

    def kernel(dq_ref, dkv_ref, *refs):
        w, (h_ref, dm_ref, o_ref, da_s) = refs[:parts], refs[parts:]

        def part(ref, col, start, width, n, e):
            got, left = None, width
            while left:
                p, at = divmod(start, CHUNK)
                take = min(CHUNK - at, left)
                one = _dot(ref[:, col : col + take], w[p][n:e, at : at + take], 1, 1)
                got = one if got is None else got + one
                col, start, left = col + take, start + take, left - take
            return got.astype(LOW).astype(F32)

        for n, e in _spans(d):
            by_q = part(dq_ref, 0, 0, nq, n, e)
            by_k = part(dkv_ref, 0, nq, nk, n, e)
            by_v = part(dkv_ref, nk, nq + nk, nk, n, e)
            da_s[:, n:e] = ((by_v + by_k).astype(LOW).astype(F32) + by_q).astype(LOW).astype(F32)
        o_ref[...] = (dm_ref[...].astype(F32) + _norm_back(da_s[...], h_ref[...].astype(F32)).astype(F32)).astype(LOW)

    return _call(kernel, m // bm, [_rows(bm, nq), _rows(bm, 2 * nk)] + [_whole((d, CHUNK), 0, n) for n in range(parts)] + [_rows(bm, d)] * 2,
                 [((m, d), LOW, _rows(bm, d))], [dq, dkv] + [wqo] * parts + [h, dm], 2 * m * d * (nq + 2 * nk), [pltpu.VMEM((bm, d), F32)],
                 name="input_back")[0]


def adamw(w, m, v, g):
    m = 0.9 * m + 0.1 * g
    v = 0.95 * v + 0.05 * g * g
    step = m * lax.rsqrt(v + 1e-8) + 0.1 * w
    return (w - 0.02 * step).astype(jnp.bfloat16), m, v


def then(first, *later):
    got = lax.optimization_barrier((first, *later))
    return got


def solution(mesh):
    reps, devices = mesh.shape["rep"], mesh.shape["dp"]
    groups = [[(2 * pair + core) * devices + x for x in range(devices) for core in range(2)] for pair in range(reps // 2)]

    def gathered(block):
        half = block.shape[0] // 2
        mine = lax.dynamic_slice_in_dim(block, lax.axis_index("rep") % 2 * half, half, 0)
        return lax.all_gather(mine, ("rep", "dp"), axis=0, tiled=True, axis_index_groups=groups)

    def scattered(g):
        return lax.psum_scatter(g, "dp", scatter_dimension=0, tiled=True)

    def step(x, dy, *arrays):
        weights, ms, vs = (arrays[i : i + 7] for i in (0, 7, 14))
        wq, wk, wv, wo, wg, wu, wd = weights
        layers = wq.shape[0]
        tokens = x.shape[1]
        heads, kv = wq.shape[2] // HEAD, wk.shape[2] // HEAD
        first = (wq.shape[2] + 2 * wk.shape[2]) // CHUNK

        half = HEAD // 2
        angle = jnp.arange(tokens, dtype=F32)[:, None] * THETA ** (-jnp.arange(half, dtype=F32) / half)
        cos, sin = jnp.cos(angle), jnp.sin(angle)
        cos, sin = jnp.concatenate([cos, cos], 1), jnp.concatenate([-sin, sin], 1)

        full = []
        for n in range(layers):
            wqo = gathered(jnp.concatenate([wq[n], wk[n], wv[n], wo[n]], 1))
            full.append((wqo, gathered(jnp.concatenate([wg[n], wu[n]], 1)), gathered(wd[n])))

        h, kept = x[0], []
        for n in range(layers):
            wqo, wgu, wdn = full[n]
            a, q, k, v = project(h, wqo, cos, sin, heads, kv)
            out, lse = attend(q, k, v)
            mid, b = joined(out, wqo, first, h)
            hidden, s, t = gated(b, wgu)
            kept.append((h, a, q, k, v, out, lse, mid, b, hidden, s, t))
            if n < layers - 1:
                h = lowered(hidden, wdn, mid)

        dh, grads, due = dy[0], [None] * layers, None
        for n in reversed(range(layers)):
            wqo, wgu, wdn = full[n]
            h, a, q, k, v, out, lse, mid, b, hidden, s, t = kept[n]
            by_down = outer(hidden, [dh], 640, "outer_down")
            if due is not None:
                due, dh = then(due, dh)
                grads[n + 1][3] = due
            by_down, dh = then(by_down, dh)
            r_down = scattered(by_down)
            dg, du = hidden_back(dh, wdn, s, t)
            by_gu = outer(b, [dg, du], 256, "outer_gu")
            by_gu, dg, du = then(by_gu, dg, du)
            r_gu = scattered(by_gu)
            r_down, dg = then(r_down, dg)
            dm = mid_back(dg, du, wgu, mid, dh)
            by_o = outer(out, [dm], 512, "outer_o")
            by_o, dm = then(by_o, dm)
            r_o = scattered(by_o)
            do = out_back(dm, wqo, first)
            dq, dkv = attend_back(q, k, v, do, out, lse, cos, sin)
            r_gu, dq = then(r_gu, dq)
            by_qkv = outer(a, [dq, dkv], 512, "outer_qkv")
            by_qkv, dq, dkv = then(by_qkv, dq, dkv)
            r_qkv = scattered(by_qkv)
            if n > 0:
                dh = input_back(dq, dkv, wqo, h, dm)
                r_o, dh = then(r_o, dh)
            due = r_qkv
            grads[n] = [r_down, r_gu, r_o, r_qkv]

        nq, nk, f = wq.shape[2], wk.shape[2], wg.shape[2]
        grads = [(r_qkv[:, :nq], r_qkv[:, nq : nq + nk], r_qkv[:, nq + nk :], r_o, r_gu[:, :f], r_gu[:, f:], r_down)
                 for r_down, r_gu, r_o, r_qkv in grads]

        new = []
        for i in range(7):
            g = jnp.stack([grads[n][i] for n in range(layers)]).astype(F32)
            new.append(adamw(weights[i].astype(F32), ms[i], vs[i], g))
        return tuple(one[which] for which in range(3) for one in new)

    states, cut = P(("rep", "dp"), None, None), P(None, "dp", None)
    return jax.shard_map(
        step,
        mesh=mesh,
        in_specs=(states, states) + (cut,) * 21,
        out_specs=(P("rep", "dp", None),) * 21,
        check_vma=False,
    )
```

```python
import jax
import jax.numpy as jnp
from jax import lax
from jax.experimental import pallas as pl
from jax.experimental.pallas import tpu as pltpu
from jax.sharding import PartitionSpec as P

HEAD = 128
THETA = 10000
LOW = jnp.bfloat16
F32 = jnp.float32
NEG = -1e30
HIDDEN = 2 * NEG
LOG2E = 1.4426950408889634
VMEM = 60 * 2**20
CHUNK = 512


def _dot(a, b, ca=1, cb=0):
    return lax.dot_general(a, b, (((ca,), (cb,)), ((), ())), preferred_element_type=F32)


def _spans(size, width=CHUNK):
    return [(n, min(n + width, size)) for n in range(0, size, width)]


def _call(kernel, grid, ins, outs, args, flops, scratch=(), name=None):
    size = sum(a.size * a.dtype.itemsize for a in args)
    got = pl.pallas_call(
        kernel,
        grid=(grid,),
        in_specs=ins,
        out_specs=[o[2] for o in outs],
        out_shape=[jax.ShapeDtypeStruct(o[0], o[1]) for o in outs],
        scratch_shapes=list(scratch),
        compiler_params=pltpu.CompilerParams(dimension_semantics=("arbitrary",), vmem_limit_bytes=VMEM),
        cost_estimate=pl.CostEstimate(flops=int(flops), transcendentals=0, bytes_accessed=size),
        name=name,
    )(*args)
    return got


def _rows(bm, width, col=0):
    return pl.BlockSpec((bm, width), lambda i, c=col: (i, c))


def _whole(shape, row=0, col=0):
    return pl.BlockSpec(shape, lambda i, r=row, c=col: (r, c), pipeline_mode=pl.Buffered(1))


def _scale(wide):
    return lax.rsqrt(jnp.mean(wide**2, -1, keepdims=True) + 1e-6)


def _norm_back(ct, wide):
    scale = _scale(wide)
    return (ct * scale - wide * (scale * scale * scale * jnp.mean(ct * wide, -1, keepdims=True))).astype(LOW)


def _turn(t, cos, sin):
    t = t.astype(F32)
    return (t * cos + pltpu.roll(t, HEAD // 2, 1) * sin).astype(LOW)


def project(h, wqo, cos, sin, heads, kv, bm=512):
    m, d = h.shape
    nq, nk = heads * HEAD, kv * HEAD
    parts = (nq + 2 * nk) // CHUNK

    def kernel(h_ref, *refs):
        w, (cos_ref, sin_ref, a_ref, q_ref, k_ref, v_ref) = refs[:parts], refs[parts:]
        wide = h_ref[...].astype(F32)
        a = (wide * _scale(wide)).astype(LOW)
        a_ref[...] = a
        cos, sin = cos_ref[...], sin_ref[...]
        for n in range(parts):
            got = _dot(a, w[n][...]).astype(LOW)
            for c in range(0, CHUNK, HEAD):
                at, t = n * CHUNK + c, got[:, c : c + HEAD]
                if at < nq:
                    q_ref[:, at : at + HEAD] = _turn(t, cos, sin)
                elif at < nq + nk:
                    k_ref[:, at - nq : at - nq + HEAD] = _turn(t, cos, sin)
                else:
                    v_ref[:, at - nq - nk : at - nq - nk + HEAD] = t

    return _call(
        kernel, m // bm,
        [_rows(bm, d)] + [_whole((d, CHUNK), 0, n) for n in range(parts)] + [_rows(bm, HEAD)] * 2,
        [((m, d), LOW, _rows(bm, d)), ((m, nq), LOW, _rows(bm, nq)), ((m, nk), LOW, _rows(bm, nk)), ((m, nk), LOW, _rows(bm, nk))],
        [h] + [wqo] * parts + [cos, sin], 2 * m * d * (nq + 2 * nk), name="project")


def _gap(bk, bq):
    return lax.broadcasted_iota(jnp.int32, (bk, bq), 1) - lax.broadcasted_iota(jnp.int32, (bk, bq), 0)


def attend(q, k, v, bq=256, bk=512):
    m, nq = q.shape
    heads, kv = nq // HEAD, k.shape[1] // HEAD
    g = heads // kv
    scale = HEAD**-0.5
    e = scale * LOG2E

    def kernel(q_ref, k_ref, v_ref, o_ref, lse_ref, top_s, mix_s, gap_s):
        iq = pl.program_id(0)

        @pl.when(iq == 0)
        def _():
            gap_s[...] = _gap(bk, bq)

        top_s[...] = jnp.full(top_s.shape, NEG, F32)
        mix_s[...] = jnp.zeros(mix_s.shape, F32)
        ones = jnp.ones((8, bk), LOW)

        def block(j, masked):
            here = pl.ds(pl.multiple_of(j * bk, bk), bk)
            scores = [_dot(k_ref[here, n // g * HEAD : (n // g + 1) * HEAD], q_ref[:, n * HEAD : (n + 1) * HEAD], 1, 1) for n in range(heads)]
            ok = gap_s[...] >= j * bk - iq * bq if masked else None
            weights, keeps = [], []
            for n, s in enumerate(scores):
                if masked:
                    s = jnp.where(ok, s, HIDDEN)
                old = top_s[n : n + 1, :]
                top = jnp.maximum(old, s.max(axis=0, keepdims=True))
                top_s[n : n + 1, :] = top
                weights.append(jnp.exp2((s - top) * e).astype(LOW))
                keeps.append(jnp.exp2((old - top) * e))
            values = [jnp.concatenate([v_ref[here, i * HEAD : (i + 1) * HEAD].T, ones], axis=0) for i in range(kv)]
            for n in range(heads):
                mix_s[n] = mix_s[n] * keeps[n] + _dot(values[n // g], weights[n], 1, 0)

        whole = iq * bq // bk
        lax.fori_loop(0, whole, lambda j, _: block(j, False), None)
        block(whole, True)
        for n in range(heads):
            total = mix_s[n, HEAD : HEAD + 1, :]
            o_ref[:, n * HEAD : (n + 1) * HEAD] = (mix_s[n, :HEAD, :] * (1 / total)).T.astype(LOW)
            lse_ref[n : n + 1, :] = top_s[n : n + 1, :] * scale + jnp.log(total)

    return _call(
        kernel, m // bq,
        [_rows(bq, nq), _whole((m, kv * HEAD)), _whole((m, kv * HEAD))],
        [((m, nq), LOW, _rows(bq, nq)), ((heads, m), F32, pl.BlockSpec((heads, bq), lambda i: (0, i)))],
        [q, k, v], 8 * m * m * nq,
        [pltpu.VMEM((heads, bq), F32), pltpu.VMEM((heads, HEAD + 8, bq), F32), pltpu.VMEM((bk, bq), jnp.int32)], name="attend")


def joined(out, wqo, first, h, bm=512):
    m, d = h.shape
    k = out.shape[1]
    parts = d // CHUNK

    def kernel(o_ref, *refs):
        w, (h_ref, mid_ref, b_ref) = refs[:parts], refs[parts:]
        o = o_ref[...]
        for n in range(parts):
            at = slice(n * CHUNK, (n + 1) * CHUNK)
            mid_ref[:, at] = (h_ref[:, at].astype(F32) + _dot(o, w[n][...]).astype(LOW).astype(F32)).astype(LOW)
        wide = mid_ref[...].astype(F32)
        b_ref[...] = (wide * _scale(wide)).astype(LOW)

    return _call(
        kernel, m // bm,
        [_rows(bm, k)] + [_whole((k, CHUNK), 0, first + n) for n in range(parts)] + [_rows(bm, d)],
        [((m, d), LOW, _rows(bm, d))] * 2, [out] + [wqo] * parts + [h], 2 * m * k * d, name="joined")


def gated(b, wgu, bm=256):
    m, d = b.shape
    f = wgu.shape[1] // 2

    def kernel(b_ref, wg_ref, wu_ref, x_ref, s_ref, t_ref):
        b = b_ref[...]
        for n, e in _spans(f):
            gate, up = _dot(b, wg_ref[:, n:e]), _dot(b, wu_ref[:, n:e])
            sig = jax.nn.sigmoid(gate)
            s = gate * sig
            x_ref[:, n:e] = (s * up).astype(LOW)
            s_ref[:, n:e] = s
            t_ref[:, n:e] = up * (sig * (1 + gate * (1 - sig)))

    return _call(
        kernel, m // bm, [_rows(bm, d), _whole((d, f), 0, 0), _whole((d, f), 0, 1)],
        [((m, f), LOW, _rows(bm, f)), ((m, f), F32, _rows(bm, f)), ((m, f), F32, _rows(bm, f))], [b, wgu, wgu], 4 * m * d * f, name="gated")


def lowered(x, w, h, bm=512):
    m, f = x.shape
    d = h.shape[1]

    def kernel(x_ref, w_ref, h_ref, o_ref):
        x = x_ref[...]
        for n, e in _spans(d):
            o_ref[:, n:e] = (h_ref[:, n:e].astype(F32) + _dot(x, w_ref[:, n:e]).astype(LOW).astype(F32)).astype(LOW)

    return _call(kernel, m // bm, [_rows(bm, f), _whole((f, d)), _rows(bm, d)], [((m, d), LOW, _rows(bm, d))], [x, w, h], 2 * m * f * d,
                 name="lowered")[0]


def placed(place, parts):
    rows, width = sum(p.shape[0] for p in parts), parts[0].shape[1]

    def kernel(place_ref, *refs):
        for i, ref in enumerate(refs[:-1]):
            refs[-1][pl.ds(pl.multiple_of(place_ref[i], HEAD), ref.shape[0]), :] = ref[...]

    return _call(kernel, 1, [pl.BlockSpec(memory_space=pltpu.SMEM)] + [_whole(p.shape) for p in parts],
                 [((rows, width), parts[0].dtype, pl.BlockSpec((rows, width), lambda i: (0, 0)))], [place, *parts], 2 * rows * width,
                 name="placed")[0]


def outer(a, bs, bm, name):
    t, k = a.shape
    widths = [b.shape[1] for b in bs]
    n = sum(widths)

    def kernel(a_ref, *refs):
        o_ref = refs[-1]
        at = a_ref[...].T
        col = 0
        for b_ref, width in zip(refs, widths):
            for c, e in _spans(width):
                o_ref[:, col + c : col + e] = _dot(at, b_ref[:, c:e]).astype(LOW)
            col += width

    return _call(kernel, k // bm, [pl.BlockSpec((t, bm), lambda i: (0, i))] + [_whole((t, w)) for w in widths],
                 [((k, n), LOW, _rows(bm, n))], [a, *bs], 2 * t * k * n, name=name)[0]


def hidden_back(dh, w, s, t, bm=256):
    m, d = dh.shape
    f = w.shape[0]

    def kernel(dh_ref, w_ref, s_ref, t_ref, dg_ref, du_ref):
        dh = dh_ref[...]
        for n, e in _spans(f):
            dx = _dot(dh, w_ref[n:e, :], 1, 1).astype(LOW).astype(F32)
            dg_ref[:, n:e] = (dx * t_ref[:, n:e]).astype(LOW)
            du_ref[:, n:e] = (dx * s_ref[:, n:e]).astype(LOW)

    return _call(kernel, m // bm, [_rows(bm, d), _whole((f, d)), _rows(bm, f), _rows(bm, f)],
                 [((m, f), LOW, _rows(bm, f)), ((m, f), LOW, _rows(bm, f))], [dh, w, s, t], 2 * m * d * f, name="hidden_back")


def mid_back(dg, du, wgu, mid, dh, bm=256):
    m, f = dg.shape
    d = mid.shape[1]

    def kernel(dg_ref, du_ref, wg_ref, wu_ref, mid_ref, dh_ref, o_ref, db_s):
        dg, du = dg_ref[...], du_ref[...]
        for n, e in _spans(d):
            one, two = _dot(dg, wg_ref[n:e, :], 1, 1).astype(LOW).astype(F32), _dot(du, wu_ref[n:e, :], 1, 1).astype(LOW).astype(F32)
            db_s[:, n:e] = (one + two).astype(LOW).astype(F32)
        o_ref[...] = (dh_ref[...].astype(F32) + _norm_back(db_s[...], mid_ref[...].astype(F32)).astype(F32)).astype(LOW)

    return _call(kernel, m // bm, [_rows(bm, f)] * 2 + [_whole((d, f), 0, 0), _whole((d, f), 0, 1)] + [_rows(bm, d)] * 2,
                 [((m, d), LOW, _rows(bm, d))], [dg, du, wgu, wgu, mid, dh], 4 * m * f * d, [pltpu.VMEM((bm, d), F32)], name="mid_back")[0]


def out_back(dm, wqo, first, bm=512):
    m, d = dm.shape
    k = wqo.shape[0]
    parts = d // CHUNK

    def kernel(dm_ref, *refs):
        w, o_ref = refs[:parts], refs[parts]
        dm = dm_ref[...]
        for n, e in _spans(k):
            o_ref[:, n:e] = sum(_dot(dm[:, p * CHUNK : (p + 1) * CHUNK], w[p][n:e, :], 1, 1) for p in range(parts)).astype(LOW)

    return _call(kernel, m // bm, [_rows(bm, d)] + [_whole((k, CHUNK), 0, first + n) for n in range(parts)],
                 [((m, k), LOW, _rows(bm, k))], [dm] + [wqo] * parts, 2 * m * k * d, name="out_back")[0]


def attend_back(q, k, v, do, out, lse, cos, sin, bq=512, bk=512):
    m, nq = q.shape
    nk = k.shape[1]
    heads, kv = nq // HEAD, nk // HEAD
    g = heads // kv
    cols = g * bq
    scale = HEAD**-0.5
    e = scale * LOG2E
    wide = min(cols, 512)
    pieces = [(i, at) for i in range(kv) for at in range(0, cols, wide)]

    def kernel(q_ref, k_ref, v_ref, do_ref, o_ref, lse_ref, cos_ref, sin_ref, dq_ref, dkv_ref, q_s, do_s, lse_s, delta_s, dq_s, dk_s, dv_s, gap_s):
        iq = pl.program_id(0)

        @pl.when(iq == 0)
        def _():
            gap_s[...] = lax.rem(lax.broadcasted_iota(jnp.int32, (bk, wide), 1), bq) - lax.broadcasted_iota(jnp.int32, (bk, wide), 0)
            dk_s[...] = jnp.zeros(dk_s.shape, F32)
            dv_s[...] = jnp.zeros(dv_s.shape, F32)

        dq_s[...] = jnp.zeros(dq_s.shape, F32)
        for n in range(heads):
            i, at = n // g, n % g * bq
            head = slice(n * HEAD, (n + 1) * HEAD)
            q_s[i, at : at + bq, :] = q_ref[:, head]
            do = do_ref[:, head]
            do_s[i, at : at + bq, :] = do
            lse_s[i : i + 1, at : at + bq] = lse_ref[n : n + 1, :] * LOG2E
            delta_s[i : i + 1, at : at + bq] = (do.astype(F32) * o_ref[:, head].astype(F32)).T.sum(axis=0, keepdims=True)

        def block(j, masked):
            here = pl.ds(pl.multiple_of(j * bk, bk), bk)
            ks = [k_ref[here, i * HEAD : (i + 1) * HEAD] for i in range(kv)]
            vs = [v_ref[here, i * HEAD : (i + 1) * HEAD] for i in range(kv)]
            qs = [q_s[i, at : at + wide, :] for i, at in pieces]
            dos = [do_s[i, at : at + wide, :] for i, at in pieces]
            scores = [_dot(ks[i], x, 1, 1) for (i, _), x in zip(pieces, qs)]
            dps = [_dot(vs[i], x, 1, 1) for (i, _), x in zip(pieces, dos)]
            ok = gap_s[...] >= j * bk - iq * bq if masked else None
            for n, (i, at) in enumerate(pieces):
                p = jnp.exp2(scores[n] * e - lse_s[i : i + 1, at : at + wide])
                if masked:
                    p = jnp.where(ok, p, 0.0)
                ds = (p * (dps[n] - delta_s[i : i + 1, at : at + wide])).astype(LOW)
                dv_s[i, here, :] += _dot(p.astype(LOW), dos[n], 1, 0)
                dk_s[i, here, :] += _dot(ds, qs[n], 1, 0)
                dq_s[i, :, at : at + wide] += _dot(ks[i].T, ds, 1, 0)

        whole = iq * bq // bk
        lax.fori_loop(0, whole, lambda j, _: block(j, False), None)
        block(whole, True)
        place = pl.ds(pl.multiple_of(iq * bq, bq), bq)
        cos, sin = cos_ref[place, :], sin_ref[place, :]
        for n in range(heads):
            i, at = n // g, n % g * bq
            dq_ref[:, n * HEAD : (n + 1) * HEAD] = _turn((dq_s[i, :, at : at + bq] * scale).T.astype(LOW), cos, -sin)

        @pl.when(iq == pl.num_programs(0) - 1)
        def _():
            for i in range(kv):
                dkv_ref[:, i * HEAD : (i + 1) * HEAD] = _turn((dk_s[i] * scale).astype(LOW), cos_ref[...], -sin_ref[...])
                dkv_ref[:, nk + i * HEAD : nk + (i + 1) * HEAD] = dv_s[i].astype(LOW)

    return _call(
        kernel, m // bq,
        [_rows(bq, nq), _whole((m, nk)), _whole((m, nk)), _rows(bq, nq), _rows(bq, nq), pl.BlockSpec((heads, bq), lambda i: (0, i)),
         _whole((m, HEAD)), _whole((m, HEAD))],
        [((m, nq), LOW, _rows(bq, nq)), ((m, 2 * nk), LOW, pl.BlockSpec((m, 2 * nk), lambda i: (0, 0)))],
        [q, k, v, do, out, lse, cos, sin], 14 * m * m * nq,
        [pltpu.VMEM((kv, cols, HEAD), LOW), pltpu.VMEM((kv, cols, HEAD), LOW), pltpu.VMEM((kv, cols), F32), pltpu.VMEM((kv, cols), F32),
         pltpu.VMEM((kv, HEAD, cols), F32), pltpu.VMEM((kv, m, HEAD), F32), pltpu.VMEM((kv, m, HEAD), F32), pltpu.VMEM((bk, wide), jnp.int32)],
        name="attend_back")


def input_back(dq, dkv, wqo, h, dm, bm=512):
    m, d = h.shape
    nq, nk = dq.shape[1], dkv.shape[1] // 2
    parts = (nq + 2 * nk) // CHUNK

    def kernel(dq_ref, dkv_ref, *refs):
        w, (h_ref, dm_ref, o_ref, da_s) = refs[:parts], refs[parts:]

        def part(ref, col, start, width, n, e):
            got, left = None, width
            while left:
                p, at = divmod(start, CHUNK)
                take = min(CHUNK - at, left)
                one = _dot(ref[:, col : col + take], w[p][n:e, at : at + take], 1, 1)
                got = one if got is None else got + one
                col, start, left = col + take, start + take, left - take
            return got.astype(LOW).astype(F32)

        for n, e in _spans(d):
            by_q = part(dq_ref, 0, 0, nq, n, e)
            by_k = part(dkv_ref, 0, nq, nk, n, e)
            by_v = part(dkv_ref, nk, nq + nk, nk, n, e)
            da_s[:, n:e] = ((by_v + by_k).astype(LOW).astype(F32) + by_q).astype(LOW).astype(F32)
        o_ref[...] = (dm_ref[...].astype(F32) + _norm_back(da_s[...], h_ref[...].astype(F32)).astype(F32)).astype(LOW)

    return _call(kernel, m // bm, [_rows(bm, nq), _rows(bm, 2 * nk)] + [_whole((d, CHUNK), 0, n) for n in range(parts)] + [_rows(bm, d)] * 2,
                 [((m, d), LOW, _rows(bm, d))], [dq, dkv] + [wqo] * parts + [h, dm], 2 * m * d * (nq + 2 * nk), [pltpu.VMEM((bm, d), F32)],
                 name="input_back")[0]


def adamw(w, m, v, g):
    m = 0.9 * m + 0.1 * g
    v = 0.95 * v + 0.05 * g * g
    step = m * lax.rsqrt(v + 1e-8) + 0.1 * w
    return (w - 0.02 * step).astype(jnp.bfloat16), m, v


def then(first, *later):
    got = lax.optimization_barrier((first, *later))
    return got


def solution(mesh):
    reps, devices = mesh.shape["rep"], mesh.shape["dp"]
    groups = [[(2 * pair + core) * devices + x for x in range(devices) for core in range(2)] for pair in range(reps // 2)]

    def gathered(block):
        half = block.shape[0] // 2
        mine = lax.dynamic_slice_in_dim(block, lax.axis_index("rep") % 2 * half, half, 0)
        return lax.all_gather(mine, ("rep", "dp"), axis=0, tiled=True, axis_index_groups=groups)

    everyone = [(rep, x) for rep in range(reps) for x in range(devices)]
    number = lambda rep, x: rep * devices + x % devices
    hop = [(number(rep, x), number(rep, x + 1 - rep % 2 * 2)) for rep, x in everyone]
    swap = [(number(rep, x), number(rep + 1 - rep % 2 * 2, x)) for rep, x in everyone]

    axes = ("rep", "dp")

    def hopped(block):
        return lax.ppermute(block, axes, hop)

    def half_of(near):
        half = near.shape[0] // 2
        return lax.dynamic_slice_in_dim(near, lax.axis_index("rep") % 2 * half, half, 0)

    def swapped(*parts):
        return [lax.ppermute(p, axes, swap) for p in parts]

    def whole(block, near, far, near2, far2):
        core, x, rows = lax.axis_index("rep") % 2, lax.axis_index("dp"), block.shape[0]
        half = rows // 2
        side = 1 - 2 * core
        at = lambda place: (place + devices) % devices * rows
        place = jnp.stack([at(x), at(x - side), at(x + side), at(x + 2) + core * half, at(x + 2) + (1 - core) * half])
        return placed(place.astype(jnp.int32), [block, near, near2, far, far2])

    def scattered(g):
        return lax.psum_scatter(g, "dp", scatter_dimension=0, tiled=True)

    def step(x, dy, *arrays):
        weights, ms, vs = (arrays[i : i + 7] for i in (0, 7, 14))
        wq, wk, wv, wo, wg, wu, wd = weights
        layers = wq.shape[0]
        tokens = x.shape[1]
        heads, kv = wq.shape[2] // HEAD, wk.shape[2] // HEAD
        first = (wq.shape[2] + 2 * wk.shape[2]) // CHUNK

        half = HEAD // 2
        angle = jnp.arange(tokens, dtype=F32)[:, None] * THETA ** (-jnp.arange(half, dtype=F32) / half)
        cos, sin = jnp.cos(angle), jnp.sin(angle)
        cos, sin = jnp.concatenate([cos, cos], 1), jnp.concatenate([-sin, sin], 1)

        block = jnp.concatenate([wq[0], wk[0], wv[0]], 1)
        near = hopped(block)
        near, wo_block = then(near, wo[0])
        far = hopped(half_of(near))
        qkv = whole(block, near, far, *swapped(near, far))
        wo_near = hopped(wo_block)
        parts, got = [], near
        for n in range(layers):
            gu, dn = jnp.concatenate([wg[n], wu[n]], 1), wd[n]
            if n == 0:
                got, gu = then(got, gu)
            parts.append((gathered(gu), gathered(dn)))

        h, kept, full, at_wo = x[0], [], [], 0
        wo_near, h = then(wo_near, h)
        wo_far = hopped(half_of(wo_near))
        for n in range(layers):
            more = n + 1 < layers
            a, q, k, v = project(h, qkv, cos, sin, heads, kv)
            if n == 0:
                q, wo_near, wo_far = then(q, wo_near, wo_far)
                wo_other = swapped(wo_near, wo_far)
            if more:
                block = jnp.concatenate([wq[n + 1], wk[n + 1], wv[n + 1], wo[n + 1]], 1)
                q, block = then(q, block)
                near = hopped(block)
            out, lse = attend(q, k, v)
            if n == 0:
                wo_n = whole(wo_block, wo_near, wo_far, *wo_other)
            if more:
                out, near = then(out, near)
                far = hopped(half_of(near))
            mid, b = joined(out, wo_n, at_wo, h)
            wgu, wdn = parts[n]
            hidden, s, t = gated(b, wgu)
            kept.append((h, a, q, k, v, out, lse, mid, b, hidden, s, t))
            full.append((qkv, (wo_n, at_wo), wgu, wdn))
            if more:
                hidden, near, far = then(hidden, near, far)
                other = swapped(near, far)
                h = lowered(hidden, wdn, mid)
                qkv = wo_n = whole(block, near, far, *other)
                at_wo = first

        dh, grads, due = dy[0], [None] * layers, None
        for n in reversed(range(layers)):
            qkv, wo_n, wgu, wdn = full[n]
            h, a, q, k, v, out, lse, mid, b, hidden, s, t = kept[n]
            by_down = outer(hidden, [dh], 640, "outer_down")
            by_down, dh = then(by_down, dh)
            r_down = scattered(by_down)
            dg, du = hidden_back(dh, wdn, s, t)
            by_gu = outer(b, [dg, du], 256, "outer_gu")
            by_gu, dg, du = then(by_gu, dg, du)
            if due is not None:
                grads[n + 1][3], dg = then(due, dg)
            r_gu = scattered(by_gu)
            r_down, dg = then(r_down, dg)
            dm = mid_back(dg, du, wgu, mid, dh)
            by_o = outer(out, [dm], 512, "outer_o")
            by_o, dm = then(by_o, dm)
            r_o = scattered(by_o)
            do = out_back(dm, *wo_n)
            dq, dkv = attend_back(q, k, v, do, out, lse, cos, sin)
            r_gu, dq = then(r_gu, dq)
            by_qkv = outer(a, [dq, dkv], 512, "outer_qkv")
            by_qkv, dq, dkv = then(by_qkv, dq, dkv)
            r_qkv = scattered(by_qkv)
            if n > 0:
                dh = input_back(dq, dkv, qkv, h, dm)
                r_o, dh = then(r_o, dh)
            due = r_qkv
            grads[n] = [r_down, r_gu, r_o, r_qkv]

        nq, nk, f = wq.shape[2], wk.shape[2], wg.shape[2]
        grads = [(r_qkv[:, :nq], r_qkv[:, nq : nq + nk], r_qkv[:, nq + nk :], r_o, r_gu[:, :f], r_gu[:, f:], r_down)
                 for r_down, r_gu, r_o, r_qkv in grads]

        new = []
        for i in range(7):
            g = jnp.stack([grads[n][i] for n in range(layers)]).astype(F32)
            new.append(adamw(weights[i].astype(F32), ms[i], vs[i], g))
        return tuple(one[which] for which in range(3) for one in new)

    states, cut = P(("rep", "dp"), None, None), P(None, "dp", None)
    return jax.shard_map(
        step,
        mesh=mesh,
        in_specs=(states, states) + (cut,) * 21,
        out_specs=(P("rep", "dp", None),) * 21,
        check_vma=False,
    )
```

```python
import jax
import jax.numpy as jnp
from jax import lax
from jax.experimental import pallas as pl
from jax.experimental.pallas import tpu as pltpu
from jax.sharding import PartitionSpec as P

HEAD = 128
THETA = 10000
LOW = jnp.bfloat16
F32 = jnp.float32
NEG = -1e30
HIDDEN = 2 * NEG
LOG2E = 1.4426950408889634
VMEM = 60 * 2**20
CHUNK = 512


def _dot(a, b, ca=1, cb=0):
    return lax.dot_general(a, b, (((ca,), (cb,)), ((), ())), preferred_element_type=F32)


def _spans(size, width=CHUNK):
    return [(n, min(n + width, size)) for n in range(0, size, width)]


def _call(kernel, grid, ins, outs, args, flops, scratch=(), name=None):
    size = sum(a.size * a.dtype.itemsize for a in args)
    got = pl.pallas_call(
        kernel,
        grid=(grid,),
        in_specs=ins,
        out_specs=[o[2] for o in outs],
        out_shape=[jax.ShapeDtypeStruct(o[0], o[1]) for o in outs],
        scratch_shapes=list(scratch),
        compiler_params=pltpu.CompilerParams(dimension_semantics=("arbitrary",), vmem_limit_bytes=VMEM),
        cost_estimate=pl.CostEstimate(flops=int(flops), transcendentals=0, bytes_accessed=size),
        name=name,
    )(*args)
    return got


def _rows(bm, width, col=0):
    return pl.BlockSpec((bm, width), lambda i, c=col: (i, c))


def _whole(shape, row=0, col=0):
    return pl.BlockSpec(shape, lambda i, r=row, c=col: (r, c), pipeline_mode=pl.Buffered(1))


def _scale(wide):
    return lax.rsqrt(jnp.mean(wide**2, -1, keepdims=True) + 1e-6)


def _norm_back(ct, wide):
    scale = _scale(wide)
    return (ct * scale - wide * (scale * scale * scale * jnp.mean(ct * wide, -1, keepdims=True))).astype(LOW)


def _turn(t, cos, sin):
    t = t.astype(F32)
    return (t * cos + pltpu.roll(t, HEAD // 2, 1) * sin).astype(LOW)


def project(h, wqo, cos, sin, heads, kv, bm=512):
    m, d = h.shape
    nq, nk = heads * HEAD, kv * HEAD
    parts = (nq + 2 * nk) // CHUNK

    def kernel(h_ref, *refs):
        w, (cos_ref, sin_ref, a_ref, q_ref, k_ref, v_ref) = refs[:parts], refs[parts:]
        wide = h_ref[...].astype(F32)
        a = (wide * _scale(wide)).astype(LOW)
        a_ref[...] = a
        cos, sin = cos_ref[...], sin_ref[...]
        for n in range(parts):
            got = _dot(a, w[n][...]).astype(LOW)
            for c in range(0, CHUNK, HEAD):
                at, t = n * CHUNK + c, got[:, c : c + HEAD]
                if at < nq:
                    q_ref[:, at : at + HEAD] = _turn(t, cos, sin)
                elif at < nq + nk:
                    k_ref[:, at - nq : at - nq + HEAD] = _turn(t, cos, sin)
                else:
                    v_ref[:, at - nq - nk : at - nq - nk + HEAD] = t

    return _call(
        kernel, m // bm,
        [_rows(bm, d)] + [_whole((d, CHUNK), 0, n) for n in range(parts)] + [_rows(bm, HEAD)] * 2,
        [((m, d), LOW, _rows(bm, d)), ((m, nq), LOW, _rows(bm, nq)), ((m, nk), LOW, _rows(bm, nk)), ((m, nk), LOW, _rows(bm, nk))],
        [h] + [wqo] * parts + [cos, sin], 2 * m * d * (nq + 2 * nk), name="project")


def _gap(bk, bq):
    return lax.broadcasted_iota(jnp.int32, (bk, bq), 1) - lax.broadcasted_iota(jnp.int32, (bk, bq), 0)


def attend(q, k, v, bq=512, bk=512):
    m, nq = q.shape
    heads, kv = nq // HEAD, k.shape[1] // HEAD
    g = heads // kv
    scale = HEAD**-0.5
    e = scale * LOG2E

    def kernel(q_ref, k_ref, v_ref, o_ref, lse_ref, top_s, mix_s, gap_s):
        iq = pl.program_id(0)

        @pl.when(iq == 0)
        def _():
            gap_s[...] = _gap(bk, bq)

        top_s[...] = jnp.full(top_s.shape, NEG, F32)
        mix_s[...] = jnp.zeros(mix_s.shape, F32)
        ones = jnp.ones((8, bk), LOW)

        def block(j, masked):
            here = pl.ds(pl.multiple_of(j * bk, bk), bk)
            scores = [_dot(k_ref[here, n // g * HEAD : (n // g + 1) * HEAD], q_ref[:, n * HEAD : (n + 1) * HEAD], 1, 1) for n in range(heads)]
            ok = gap_s[...] >= j * bk - iq * bq if masked else None
            weights, keeps = [], []
            for n, s in enumerate(scores):
                if masked:
                    s = jnp.where(ok, s, HIDDEN)
                old = top_s[n : n + 1, :]
                top = jnp.maximum(old, s.max(axis=0, keepdims=True))
                top_s[n : n + 1, :] = top
                weights.append(jnp.exp2((s - top) * e).astype(LOW))
                keeps.append(jnp.exp2((old - top) * e))
            values = [jnp.concatenate([v_ref[here, i * HEAD : (i + 1) * HEAD].T, ones], axis=0) for i in range(kv)]
            for n in range(heads):
                mix_s[n] = mix_s[n] * keeps[n] + _dot(values[n // g], weights[n], 1, 0)

        whole = iq * bq // bk
        lax.fori_loop(0, whole, lambda j, _: block(j, False), None)
        block(whole, True)
        for n in range(heads):
            total = mix_s[n, HEAD : HEAD + 1, :]
            o_ref[:, n * HEAD : (n + 1) * HEAD] = (mix_s[n, :HEAD, :] * (1 / total)).T.astype(LOW)
            lse_ref[n : n + 1, :] = top_s[n : n + 1, :] * scale + jnp.log(total)

    return _call(
        kernel, m // bq,
        [_rows(bq, nq), _whole((m, kv * HEAD)), _whole((m, kv * HEAD))],
        [((m, nq), LOW, _rows(bq, nq)), ((heads, m), F32, pl.BlockSpec((heads, bq), lambda i: (0, i)))],
        [q, k, v], 8 * m * m * nq,
        [pltpu.VMEM((heads, bq), F32), pltpu.VMEM((heads, HEAD + 8, bq), F32), pltpu.VMEM((bk, bq), jnp.int32)], name="attend")


def joined(out, wqo, first, h, bm=512):
    m, d = h.shape
    k = out.shape[1]
    parts = d // CHUNK

    def kernel(o_ref, *refs):
        w, (h_ref, mid_ref, b_ref) = refs[:parts], refs[parts:]
        o = o_ref[...]
        for n in range(parts):
            at = slice(n * CHUNK, (n + 1) * CHUNK)
            mid_ref[:, at] = (h_ref[:, at].astype(F32) + _dot(o, w[n][...]).astype(LOW).astype(F32)).astype(LOW)
        wide = mid_ref[...].astype(F32)
        b_ref[...] = (wide * _scale(wide)).astype(LOW)

    return _call(
        kernel, m // bm,
        [_rows(bm, k)] + [_whole((k, CHUNK), 0, first + n) for n in range(parts)] + [_rows(bm, d)],
        [((m, d), LOW, _rows(bm, d))] * 2, [out] + [wqo] * parts + [h], 2 * m * k * d, name="joined")


def gated(b, wgu, bm=256):
    m, d = b.shape
    f = wgu.shape[1] // 2

    def kernel(b_ref, wg_ref, wu_ref, x_ref, s_ref, t_ref):
        b = b_ref[...]
        for n, e in _spans(f):
            gate, up = _dot(b, wg_ref[:, n:e]), _dot(b, wu_ref[:, n:e])
            sig = jax.nn.sigmoid(gate)
            s = gate * sig
            x_ref[:, n:e] = (s * up).astype(LOW)
            s_ref[:, n:e] = s
            t_ref[:, n:e] = up * (sig * (1 + gate * (1 - sig)))

    return _call(
        kernel, m // bm, [_rows(bm, d), _whole((d, f), 0, 0), _whole((d, f), 0, 1)],
        [((m, f), LOW, _rows(bm, f)), ((m, f), F32, _rows(bm, f)), ((m, f), F32, _rows(bm, f))], [b, wgu, wgu], 4 * m * d * f, name="gated")


def lowered(x, w, h, bm=512):
    m, f = x.shape
    d = h.shape[1]

    def kernel(x_ref, w_ref, h_ref, o_ref):
        x = x_ref[...]
        for n, e in _spans(d):
            o_ref[:, n:e] = (h_ref[:, n:e].astype(F32) + _dot(x, w_ref[:, n:e]).astype(LOW).astype(F32)).astype(LOW)

    return _call(kernel, m // bm, [_rows(bm, f), _whole((f, d)), _rows(bm, d)], [((m, d), LOW, _rows(bm, d))], [x, w, h], 2 * m * f * d,
                 name="lowered")[0]


def placed(place, parts):
    rows, width = sum(p.shape[0] for p in parts), parts[0].shape[1]

    def kernel(place_ref, *refs):
        for i, ref in enumerate(refs[:-1]):
            refs[-1][pl.ds(pl.multiple_of(place_ref[i], HEAD), ref.shape[0]), :] = ref[...]

    return _call(kernel, 1, [pl.BlockSpec(memory_space=pltpu.SMEM)] + [_whole(p.shape) for p in parts],
                 [((rows, width), parts[0].dtype, pl.BlockSpec((rows, width), lambda i: (0, 0)))], [place, *parts], 2 * rows * width,
                 name="placed")[0]


def outer(a, bs, bm, name):
    t, k = a.shape
    widths = [b.shape[1] for b in bs]
    n = sum(widths)

    def kernel(a_ref, *refs):
        o_ref = refs[-1]
        at = a_ref[...].T
        col = 0
        for b_ref, width in zip(refs, widths):
            for c, e in _spans(width):
                o_ref[:, col + c : col + e] = _dot(at, b_ref[:, c:e]).astype(LOW)
            col += width

    return _call(kernel, k // bm, [pl.BlockSpec((t, bm), lambda i: (0, i))] + [_whole((t, w)) for w in widths],
                 [((k, n), LOW, _rows(bm, n))], [a, *bs], 2 * t * k * n, name=name)[0]


def hidden_back(dh, w, s, t, bm=256):
    m, d = dh.shape
    f = w.shape[0]

    def kernel(dh_ref, w_ref, s_ref, t_ref, dg_ref, du_ref):
        dh = dh_ref[...]
        for n, e in _spans(f):
            dx = _dot(dh, w_ref[n:e, :], 1, 1).astype(LOW).astype(F32)
            dg_ref[:, n:e] = (dx * t_ref[:, n:e]).astype(LOW)
            du_ref[:, n:e] = (dx * s_ref[:, n:e]).astype(LOW)

    return _call(kernel, m // bm, [_rows(bm, d), _whole((f, d)), _rows(bm, f), _rows(bm, f)],
                 [((m, f), LOW, _rows(bm, f)), ((m, f), LOW, _rows(bm, f))], [dh, w, s, t], 2 * m * d * f, name="hidden_back")


def hidden_and_outer(dh, w, s, t, b, shards, bf=640):
    m, d = dh.shape
    f = w.shape[0]
    rows = d // shards

    def kernel(dh_ref, w_ref, s_ref, t_ref, b_ref, dg_ref, du_ref, o_ref, bt_s):
        @pl.when(pl.program_id(0) == 0)
        def _():
            for n, e in _spans(m):
                bt_s[:, n:e] = b_ref[n:e, :].T

        for n, e in _spans(m):
            dx = _dot(dh_ref[n:e, :], w_ref[...], 1, 1).astype(LOW).astype(F32)
            dg_ref[n:e, :] = (dx * t_ref[n:e, :]).astype(LOW)
            du_ref[n:e, :] = (dx * s_ref[n:e, :]).astype(LOW)
        for p in range(shards):
            bt = bt_s[p * rows : (p + 1) * rows, :]
            o_ref[p, 0] = _dot(bt, dg_ref[...]).astype(LOW)
            o_ref[p, 1] = _dot(bt, du_ref[...]).astype(LOW)

    cols = pl.BlockSpec((m, bf), lambda i: (0, i))
    dg, du, got = _call(
        kernel, f // bf, [_whole((m, d)), pl.BlockSpec((bf, d), lambda i: (i, 0)), cols, cols, _whole((m, d))],
        [((m, f), LOW, cols), ((m, f), LOW, cols), ((shards, 2, rows, f), LOW, pl.BlockSpec((shards, 2, rows, bf), lambda i: (0, 0, 0, i)))],
        [dh, w, s, t, b], 6 * m * d * f, [pltpu.VMEM((d, m), LOW)], name="hidden_and_outer")
    return dg, du, got.reshape(2 * d, f)


def mid_back(dg, du, wgu, mid, dh, bm=256):
    m, f = dg.shape
    d = mid.shape[1]

    def kernel(dg_ref, du_ref, wg_ref, wu_ref, mid_ref, dh_ref, o_ref, db_s):
        dg, du = dg_ref[...], du_ref[...]
        for n, e in _spans(d):
            one, two = _dot(dg, wg_ref[n:e, :], 1, 1).astype(LOW).astype(F32), _dot(du, wu_ref[n:e, :], 1, 1).astype(LOW).astype(F32)
            db_s[:, n:e] = (one + two).astype(LOW).astype(F32)
        o_ref[...] = (dh_ref[...].astype(F32) + _norm_back(db_s[...], mid_ref[...].astype(F32)).astype(F32)).astype(LOW)

    return _call(kernel, m // bm, [_rows(bm, f)] * 2 + [_whole((d, f), 0, 0), _whole((d, f), 0, 1)] + [_rows(bm, d)] * 2,
                 [((m, d), LOW, _rows(bm, d))], [dg, du, wgu, wgu, mid, dh], 4 * m * f * d, [pltpu.VMEM((bm, d), F32)], name="mid_back")[0]


def out_back(dm, wqo, first, bm=512):
    m, d = dm.shape
    k = wqo.shape[0]
    parts = d // CHUNK

    def kernel(dm_ref, *refs):
        w, o_ref = refs[:parts], refs[parts]
        dm = dm_ref[...]
        for n, e in _spans(k):
            o_ref[:, n:e] = sum(_dot(dm[:, p * CHUNK : (p + 1) * CHUNK], w[p][n:e, :], 1, 1) for p in range(parts)).astype(LOW)

    return _call(kernel, m // bm, [_rows(bm, d)] + [_whole((k, CHUNK), 0, first + n) for n in range(parts)],
                 [((m, k), LOW, _rows(bm, k))], [dm] + [wqo] * parts, 2 * m * k * d, name="out_back")[0]


def attend_back(q, k, v, do, out, lse, cos, sin, bq=512, bk=512):
    m, nq = q.shape
    nk = k.shape[1]
    heads, kv = nq // HEAD, nk // HEAD
    g = heads // kv
    cols = g * bq
    scale = HEAD**-0.5
    e = scale * LOG2E
    wide = min(cols, 512)
    pieces = [(i, at) for i in range(kv) for at in range(0, cols, wide)]

    def kernel(q_ref, k_ref, v_ref, do_ref, o_ref, lse_ref, cos_ref, sin_ref, dq_ref, dkv_ref, q_s, do_s, lse_s, delta_s, dq_s, dk_s, dv_s, gap_s):
        iq = pl.program_id(0)

        @pl.when(iq == 0)
        def _():
            gap_s[...] = lax.rem(lax.broadcasted_iota(jnp.int32, (bk, wide), 1), bq) - lax.broadcasted_iota(jnp.int32, (bk, wide), 0)
            dk_s[...] = jnp.zeros(dk_s.shape, F32)
            dv_s[...] = jnp.zeros(dv_s.shape, F32)

        dq_s[...] = jnp.zeros(dq_s.shape, F32)
        for n in range(heads):
            i, at = n // g, n % g * bq
            head = slice(n * HEAD, (n + 1) * HEAD)
            q_s[i, at : at + bq, :] = q_ref[:, head]
            do = do_ref[:, head]
            do_s[i, at : at + bq, :] = do
            lse_s[i : i + 1, at : at + bq] = lse_ref[n : n + 1, :] * LOG2E
            delta_s[i : i + 1, at : at + bq] = (do.astype(F32) * o_ref[:, head].astype(F32)).T.sum(axis=0, keepdims=True)

        def block(j, masked):
            here = pl.ds(pl.multiple_of(j * bk, bk), bk)
            ks = [k_ref[here, i * HEAD : (i + 1) * HEAD] for i in range(kv)]
            vs = [v_ref[here, i * HEAD : (i + 1) * HEAD] for i in range(kv)]
            qs = [q_s[i, at : at + wide, :] for i, at in pieces]
            dos = [do_s[i, at : at + wide, :] for i, at in pieces]
            scores = [_dot(ks[i], x, 1, 1) for (i, _), x in zip(pieces, qs)]
            dps = [_dot(vs[i], x, 1, 1) for (i, _), x in zip(pieces, dos)]
            ok = gap_s[...] >= j * bk - iq * bq if masked else None
            for n, (i, at) in enumerate(pieces):
                p = jnp.exp2(scores[n] * e - lse_s[i : i + 1, at : at + wide])
                if masked:
                    p = jnp.where(ok, p, 0.0)
                ds = (p * (dps[n] - delta_s[i : i + 1, at : at + wide])).astype(LOW)
                dv_s[i, here, :] += _dot(p.astype(LOW), dos[n], 1, 0)
                dk_s[i, here, :] += _dot(ds, qs[n], 1, 0)
                dq_s[i, :, at : at + wide] += _dot(ks[i].T, ds, 1, 0)

        whole = iq * bq // bk
        lax.fori_loop(0, whole, lambda j, _: block(j, False), None)
        block(whole, True)
        place = pl.ds(pl.multiple_of(iq * bq, bq), bq)
        cos, sin = cos_ref[place, :], sin_ref[place, :]
        for n in range(heads):
            i, at = n // g, n % g * bq
            dq_ref[:, n * HEAD : (n + 1) * HEAD] = _turn((dq_s[i, :, at : at + bq] * scale).T.astype(LOW), cos, -sin)

        @pl.when(iq == pl.num_programs(0) - 1)
        def _():
            for i in range(kv):
                dkv_ref[:, i * HEAD : (i + 1) * HEAD] = _turn((dk_s[i] * scale).astype(LOW), cos_ref[...], -sin_ref[...])
                dkv_ref[:, nk + i * HEAD : nk + (i + 1) * HEAD] = dv_s[i].astype(LOW)

    return _call(
        kernel, m // bq,
        [_rows(bq, nq), _whole((m, nk)), _whole((m, nk)), _rows(bq, nq), _rows(bq, nq), pl.BlockSpec((heads, bq), lambda i: (0, i)),
         _whole((m, HEAD)), _whole((m, HEAD))],
        [((m, nq), LOW, _rows(bq, nq)), ((m, 2 * nk), LOW, pl.BlockSpec((m, 2 * nk), lambda i: (0, 0)))],
        [q, k, v, do, out, lse, cos, sin], 14 * m * m * nq,
        [pltpu.VMEM((kv, cols, HEAD), LOW), pltpu.VMEM((kv, cols, HEAD), LOW), pltpu.VMEM((kv, cols), F32), pltpu.VMEM((kv, cols), F32),
         pltpu.VMEM((kv, HEAD, cols), F32), pltpu.VMEM((kv, m, HEAD), F32), pltpu.VMEM((kv, m, HEAD), F32), pltpu.VMEM((bk, wide), jnp.int32)],
        name="attend_back")


def input_back(dq, dkv, wqo, h, dm, bm=512):
    m, d = h.shape
    nq, nk = dq.shape[1], dkv.shape[1] // 2
    parts = (nq + 2 * nk) // CHUNK

    def kernel(dq_ref, dkv_ref, *refs):
        w, (h_ref, dm_ref, o_ref, da_s) = refs[:parts], refs[parts:]

        def part(ref, col, start, width, n, e):
            got, left = None, width
            while left:
                p, at = divmod(start, CHUNK)
                take = min(CHUNK - at, left)
                one = _dot(ref[:, col : col + take], w[p][n:e, at : at + take], 1, 1)
                got = one if got is None else got + one
                col, start, left = col + take, start + take, left - take
            return got.astype(LOW).astype(F32)

        for n, e in _spans(d):
            by_q = part(dq_ref, 0, 0, nq, n, e)
            by_k = part(dkv_ref, 0, nq, nk, n, e)
            by_v = part(dkv_ref, nk, nq + nk, nk, n, e)
            da_s[:, n:e] = ((by_v + by_k).astype(LOW).astype(F32) + by_q).astype(LOW).astype(F32)
        o_ref[...] = (dm_ref[...].astype(F32) + _norm_back(da_s[...], h_ref[...].astype(F32)).astype(F32)).astype(LOW)

    return _call(kernel, m // bm, [_rows(bm, nq), _rows(bm, 2 * nk)] + [_whole((d, CHUNK), 0, n) for n in range(parts)] + [_rows(bm, d)] * 2,
                 [((m, d), LOW, _rows(bm, d))], [dq, dkv] + [wqo] * parts + [h, dm], 2 * m * d * (nq + 2 * nk), [pltpu.VMEM((bm, d), F32)],
                 name="input_back")[0]


def adamw(w, m, v, g):
    m = 0.9 * m + 0.1 * g
    v = 0.95 * v + 0.05 * g * g
    step = m * lax.rsqrt(v + 1e-8) + 0.1 * w
    return (w - 0.02 * step).astype(jnp.bfloat16), m, v


def then(first, *later):
    got = lax.optimization_barrier((first, *later))
    return got


def solution(mesh):
    reps, devices = mesh.shape["rep"], mesh.shape["dp"]
    groups = [[(2 * pair + core) * devices + x for x in range(devices) for core in range(2)] for pair in range(reps // 2)]

    def gathered(block):
        half = block.shape[0] // 2
        mine = lax.dynamic_slice_in_dim(block, lax.axis_index("rep") % 2 * half, half, 0)
        return lax.all_gather(mine, ("rep", "dp"), axis=0, tiled=True, axis_index_groups=groups)

    everyone = [(rep, x) for rep in range(reps) for x in range(devices)]
    number = lambda rep, x: rep * devices + x % devices
    hop = [(number(rep, x), number(rep, x + 1 - rep % 2 * 2)) for rep, x in everyone]
    swap = [(number(rep, x), number(rep + 1 - rep % 2 * 2, x)) for rep, x in everyone]

    axes = ("rep", "dp")

    def hopped(block):
        return lax.ppermute(block, axes, hop)

    def half_of(near):
        half = near.shape[0] // 2
        return lax.dynamic_slice_in_dim(near, lax.axis_index("rep") % 2 * half, half, 0)

    def swapped(*parts):
        return [lax.ppermute(p, axes, swap) for p in parts]

    def whole(block, near, far, near2, far2):
        core, x, rows = lax.axis_index("rep") % 2, lax.axis_index("dp"), block.shape[0]
        half = rows // 2
        side = 1 - 2 * core
        at = lambda place: (place + devices) % devices * rows
        place = jnp.stack([at(x), at(x - side), at(x + side), at(x + 2) + core * half, at(x + 2) + (1 - core) * half])
        return placed(place.astype(jnp.int32), [block, near, near2, far, far2])

    def scattered(g):
        return lax.psum_scatter(g, "dp", scatter_dimension=0, tiled=True)

    def step(x, dy, *arrays):
        weights, ms, vs = (arrays[i : i + 7] for i in (0, 7, 14))
        wq, wk, wv, wo, wg, wu, wd = weights
        layers = wq.shape[0]
        tokens = x.shape[1]
        heads, kv = wq.shape[2] // HEAD, wk.shape[2] // HEAD
        first = (wq.shape[2] + 2 * wk.shape[2]) // CHUNK

        half = HEAD // 2
        angle = jnp.arange(tokens, dtype=F32)[:, None] * THETA ** (-jnp.arange(half, dtype=F32) / half)
        cos, sin = jnp.cos(angle), jnp.sin(angle)
        cos, sin = jnp.concatenate([cos, cos], 1), jnp.concatenate([-sin, sin], 1)

        qkv = wo_n = gathered(jnp.concatenate([wq[0], wk[0], wv[0], wo[0]], 1))
        parts = [(gathered(jnp.concatenate([wg[n], wu[n]], 1)), gathered(wd[n])) for n in range(layers)]

        h, kept, full, at_wo = x[0], [], [], first
        for n in range(layers):
            more = n + 1 < layers
            a, q, k, v = project(h, qkv, cos, sin, heads, kv)
            if more:
                block = jnp.concatenate([wq[n + 1], wk[n + 1], wv[n + 1], wo[n + 1]], 1)
                q, block = then(q, block)
                near = hopped(block)
            out, lse = attend(q, k, v)
            mid, b = joined(out, wo_n, at_wo, h)
            wgu, wdn = parts[n]
            if more:
                b, near = then(b, near)
                far = hopped(half_of(near))
            hidden, s, t = gated(b, wgu)
            kept.append((h, a, q, k, v, out, lse, mid, b, hidden, s, t))
            full.append((qkv, (wo_n, at_wo), wgu, wdn))
            if more:
                hidden, near, far = then(hidden, near, far)
                other = swapped(near, far)
                h = lowered(hidden, wdn, mid)
                qkv = wo_n = whole(block, near, far, *other)

        dh, grads, due = dy[0], [None] * layers, None
        for n in reversed(range(layers)):
            qkv, wo_n, wgu, wdn = full[n]
            h, a, q, k, v, out, lse, mid, b, hidden, s, t = kept[n]
            by_down = outer(hidden, [dh], 640, "outer_down")
            by_down, dh = then(by_down, dh)
            r_down = scattered(by_down)
            dg, du, by_gu = hidden_and_outer(dh, wdn, s, t, b, devices)
            by_gu, dg, du = then(by_gu, dg, du)
            if due is not None:
                grads[n + 1][3], dg = then(due, dg)
            r_gu = scattered(by_gu)
            r_down, dg = then(r_down, dg)
            dm = mid_back(dg, du, wgu, mid, dh)
            by_o = outer(out, [dm], 512, "outer_o")
            by_o, dm = then(by_o, dm)
            r_o = scattered(by_o)
            do = out_back(dm, *wo_n)
            dq, dkv = attend_back(q, k, v, do, out, lse, cos, sin)
            r_gu, dq = then(r_gu, dq)
            by_qkv = outer(a, [dq, dkv], 512, "outer_qkv")
            by_qkv, dq, dkv = then(by_qkv, dq, dkv)
            r_qkv = scattered(by_qkv)
            if n > 0:
                dh = input_back(dq, dkv, qkv, h, dm)
                r_o, dh = then(r_o, dh)
            due = r_qkv
            grads[n] = [r_down, r_gu, r_o, r_qkv]

        nq, nk, rows = wq.shape[2], wk.shape[2], wg.shape[1]
        grads = [(r_qkv[:, :nq], r_qkv[:, nq : nq + nk], r_qkv[:, nq + nk :], r_o, r_gu[:rows], r_gu[rows:], r_down)
                 for r_down, r_gu, r_o, r_qkv in grads]

        new = []
        for i in range(7):
            g = jnp.stack([grads[n][i] for n in range(layers)]).astype(F32)
            new.append(adamw(weights[i].astype(F32), ms[i], vs[i], g))
        return tuple(one[which] for which in range(3) for one in new)

    states, cut = P(("rep", "dp"), None, None), P(None, "dp", None)
    return jax.shard_map(
        step,
        mesh=mesh,
        in_specs=(states, states) + (cut,) * 21,
        out_specs=(P("rep", "dp", None),) * 21,
        check_vma=False,
    )
```
